128 devices in a mesh: state: 16 (over y_hi, x, core), dp: 8 (over y_lo, z).
Axes of the slice: x: 4, y: 4 (y_hi: 2, y_lo: 2; y = y_hi * 2 + y_lo), z: 4, core: 2. Of those that a mesh axis runs over, the one named last changes fastest.
Arguments:
- state_ensemble: float32 [32768, 256], P('state'), may hold values from -80 to 80, as said below
- predicted_data: float32 [65536, 256], P(('state', 'dp')), may hold values from -125 to 125, as said below
- innovations: bfloat16 [65536, 256], P(('state', 'dp')), may hold values from -6 to 6
Outputs:
- increment: float32 [32768, 256], P(('state', 'dp'))
The draws below stay inside these ranges and needn't reach their ends.
Inputs may be any that keep to these rules, and one draw needn't show every extreme that they name: `state_ensemble`: finite values. `predicted_data`: finite values.
All inputs are finite; a program needn't handle non-finite values.
Results may differ from the reference program's by a relative error of at most 0.0042.
Values may be sent and summed in bfloat16 or wider, within the bound.
No kernel may reach another device: no remote copies, remote signals or barrier semaphores. Data moves between devices by JAX's collectives and lax.ppermute only.
A program may use at most 64 MiB of HBM per device.

```python
import math
import jax
import jax.numpy as jnp
from jax import lax

NE = 256
NX = 32768
ND = 65536


def joint_draw(key):
    base = jax.random.fold_in(key, 11)
    keys = jax.random.split(base, 4)
    latent = jnp.clip(jax.random.normal(keys[0], (NX, NE), jnp.float32), -6.0, 6.0)
    first = jax.random.randint(keys[1], (ND,), 0, NX)
    second = jax.random.randint(keys[2], (ND,), 0, NX)
    noise = jnp.clip(jax.random.normal(keys[3], (ND, NE), jnp.float32), -6.0, 6.0)
    data = 0.7 * latent[first] + 0.5 * latent[second] + 0.5 * noise
    state = latent
    return (state, data)


def draw_state_ensemble(key, part):
    return joint_draw(key)[0]


def draw_predicted_data(key, part):
    return joint_draw(key)[1]


def levels(own_key, shape, cuts, least, top_value):
    def one(dim, blocks):
        heights = jax.random.uniform(jax.random.fold_in(jax.random.fold_in(own_key, 6), dim), (blocks,), jnp.float32, least / len(cuts), top_value / len(cuts))
        return jnp.repeat(jnp.exp(heights), shape[dim] // blocks).reshape((-1,) + (1,) * (len(shape) - dim - 1))

    loudness = one(*cuts[0])
    for cut in cuts[1:]:
        loudness = loudness * one(*cut)
    return loudness


def centred(stream_key, dims, scale, reach, shards=(), dtype=jnp.bfloat16):
    factor_of = levels(stream_key, dims, shards, -0.22, 0.18) if shards else 1.0
    array = jax.random.normal(stream_key, dims, jnp.float32) * scale * factor_of
    return jnp.minimum(jnp.maximum(array, -reach), reach).astype(dtype)


def setup_inputs(seed: int = 0) -> dict:
    streams_of = jax.random.split(jax.random.key(seed), 4)
    return {
        "state_ensemble": draw_state_ensemble(jax.random.fold_in(streams_of[3], 71), 0),
        "predicted_data": draw_predicted_data(jax.random.fold_in(streams_of[3], 71), 0),
        "innovations": centred(streams_of[2], (ND, NE), 1.0, 6.0, ((0, 128),)),
    }


def standardize(values):
    anomalies = values - lax.optimization_barrier(jnp.mean(values, axis=1, keepdims=True))
    spread = jnp.sqrt(lax.optimization_barrier(jnp.sum(anomalies * anomalies, axis=1)) / (NE - 1) + 1e-06)
    return ((anomalies / spread[:, None]).astype(jnp.bfloat16), spread)

def reference(state_ensemble, predicted_data, innovations):
    state_std, spread = standardize(state_ensemble)
    data_std, unused = standardize(predicted_data)
    data_size = math.gcd(ND, 512)
    state_size = math.gcd(NX, 2048)
    data_blocks = data_std.astype(jnp.float32).reshape(ND // data_size, data_size, NE)
    innov_blocks = innovations.astype(jnp.float32).reshape(ND // data_size, data_size, NE)

    def per_state(rows_block):

        def advance(running, pair):
            correl = jnp.dot(rows_block, pair[0].T) / (NE - 1)
            localized = (correl * correl * correl).astype(jnp.bfloat16).astype(jnp.float32)
            return (running + jnp.dot(localized, pair[1]), None)
        start_zero = jnp.zeros((rows_block.shape[0], NE), jnp.float32)
        return lax.scan(advance, start_zero, (data_blocks, innov_blocks))[0]
    stacked = state_std.astype(jnp.float32).reshape(NX // state_size, state_size, NE)
    summed = lax.map(per_state, stacked).reshape(NX, NE)
    return spread[:, None] * summed
```

```python
import jax
import jax.numpy as jnp
from jax import lax
from jax.experimental import pallas as pl
from jax.experimental.pallas import tpu as pltpu
from jax.sharding import PartitionSpec as P


AXES = ("state", "dp")
VMEM = pl.BlockSpec(memory_space=pltpu.VMEM)
LIMIT = 24 << 20


def place(i):
    s, d = divmod(i, 8)
    y_hi, rest = divmod(s, 8)
    x, core = divmod(rest, 2)
    y_lo, z = divmod(d, 4)
    return x, y_hi * 2 + y_lo, z, core


def index(x, y, z, core):
    x, y, z = x % 4, y % 4, z % 4
    return ((y // 2) * 8 + x * 2 + core) * 8 + (y % 2) * 4 + z


def sent(value, to):
    return lax.ppermute(value, AXES, [(i, index(*to(*place(i)))) for i in range(128)])


def x_up(x, y, z, core):
    return x + 1, y, z, core


def x_down(x, y, z, core):
    return x - 1, y, z, core


def x_far(x, y, z, core):
    return x + 2, y, z, core


def y_across(x, y, z, core):
    return x, 3 - y, z, core


def other_core(x, y, z, core):
    return x, y, z, 1 - core


def standard(values):
    members = values.shape[1]
    anomalies = values - jnp.mean(values, axis=1, keepdims=True)
    spread = jnp.sqrt(jnp.sum(anomalies * anomalies, axis=1, keepdims=True) / (members - 1) + 1e-06)
    return (anomalies / spread).astype(jnp.bfloat16), spread


def cost(flops, size):
    return pl.CostEstimate(flops=flops, bytes_accessed=size, transcendentals=0)


def pack_data(predicted, innovations):
    rows, members = predicted.shape

    def body(p_ref, i_ref, o_ref):
        o_ref[:, 0:members] = standard(p_ref[...])[0]
        o_ref[:, members:] = i_ref[...]

    return pl.pallas_call(
        body,
        out_shape=jax.ShapeDtypeStruct((rows, 2 * members), jnp.bfloat16),
        in_specs=[VMEM, VMEM],
        out_specs=VMEM,
        compiler_params=pltpu.CompilerParams(vmem_limit_bytes=LIMIT),
        cost_estimate=cost(1 << 20, 1 << 20),
        name="pack_data",
    )(predicted, innovations)


def prepare_state(state, own):
    rows, members = state.shape
    tile = 256

    def body(s_ref, o_ref, w_ref):
        mine = lax.axis_index("dp")

        def step(i, _):
            part = pl.ds(pl.multiple_of(i * tile, tile), tile)
            std, spread = standard(s_ref[part, :])
            o_ref[part, :] = std

            @pl.when(i == mine)
            def _():
                w_ref[...] = jnp.broadcast_to(spread, (own, members))

            return 0

        lax.fori_loop(0, rows // tile, step, 0)

    return pl.pallas_call(
        body,
        out_shape=(
            jax.ShapeDtypeStruct((rows, members), jnp.bfloat16),
            jax.ShapeDtypeStruct((own, members), jnp.float32),
        ),
        in_specs=[VMEM],
        out_specs=(VMEM, VMEM),
        compiler_params=pltpu.CompilerParams(vmem_limit_bytes=LIMIT),
        cost_estimate=cost(1 << 24, 1 << 22),
        name="prepare_state",
    )(state)


def tile_sum(state, chunks, start, members, width=256):
    total = start
    for chunk in chunks:
        for c in range(0, chunk.shape[0], width):
            correl = lax.dot_general(
                state,
                chunk[c : c + width, 0:members],
                (((1,), (1,)), ((), ())),
                preferred_element_type=jnp.float32,
            ) * (1.0 / (members - 1))
            localized = (correl * correl * correl).astype(jnp.bfloat16)
            part = jnp.dot(localized, chunk[c : c + width, members:], preferred_element_type=jnp.float32)
            total = part if total is None else total + part
    return total


def add_chunks(running, state, chunks, name, tile=512):
    rows, members = state.shape
    count = len(chunks)
    first = running is None

    def body(*refs):
        start_ref = None if first else refs[0]
        s_ref, *x_refs = refs[0 if first else 1 : -1]
        o_ref = refs[-1]

        def step(i, _):
            part = pl.ds(pl.multiple_of(i * tile, tile), tile)
            start = None if first else start_ref[part, :]
            o_ref[part, :] = tile_sum(s_ref[part, :], x_refs, start, members)
            return 0

        lax.fori_loop(0, rows // tile, step, 0)

    operands = ([] if first else [running]) + [state, *chunks]
    return pl.pallas_call(
        body,
        out_shape=jax.ShapeDtypeStruct((rows, members), jnp.float32),
        in_specs=[VMEM] * len(operands),
        out_specs=VMEM,
        input_output_aliases={} if first else {0: 0},
        compiler_params=pltpu.CompilerParams(vmem_limit_bytes=LIMIT),
        cost_estimate=cost(4 * rows * members * 512 * count, 1 << 22),
        name=name,
    )(*operands)


def last_chunks(running, state, chunks, own, tile=512):
    rows, members = state.shape
    count = len(chunks)
    peers = rows // own

    def body(start_ref, s_ref, *refs):
        x_refs, o_refs, total_ref = refs[:count], refs[count:-1], refs[-1]
        mine = lax.axis_index("dp")
        lo, z = mine // 4, lax.rem(mine, 4)

        def step(i, _):
            part = pl.ds(pl.multiple_of(i * tile, tile), tile)
            total_ref[part, :] = tile_sum(s_ref[part, :], x_refs, start_ref[part, :], members)
            return 0

        lax.fori_loop(0, rows // tile, step, 0)
        for k in range(peers):
            to = lax.rem(lo + k // 4, 2) * 4 + lax.rem(z + k % 4, 4)
            block = total_ref[pl.ds(pl.multiple_of(to * own, own), own), :]
            o_refs[k][...] = block.astype(o_refs[k].dtype)

    operands = [running, state, *chunks]
    return pl.pallas_call(
        body,
        out_shape=[
            jax.ShapeDtypeStruct((own, members), jnp.bfloat16 if k else jnp.float32) for k in range(peers)
        ],
        in_specs=[VMEM] * len(operands),
        out_specs=[VMEM] * peers,
        scratch_shapes=[pltpu.VMEM((rows, members), jnp.float32)],
        compiler_params=pltpu.CompilerParams(vmem_limit_bytes=LIMIT),
        cost_estimate=cost(4 * rows * members * 512 * count, 1 << 22),
        name="last_chunks",
    )(*operands)


def finish(spread, own_block, blocks):
    def body(w_ref, f_ref, *refs):
        total = f_ref[...]
        for ref in refs[:-1]:
            total = total + ref[...].astype(jnp.float32)
        refs[-1][...] = w_ref[...] * total

    return pl.pallas_call(
        body,
        out_shape=jax.ShapeDtypeStruct(own_block.shape, jnp.float32),
        in_specs=[VMEM] * (2 + len(blocks)),
        out_specs=VMEM,
        compiler_params=pltpu.CompilerParams(vmem_limit_bytes=LIMIT),
        cost_estimate=cost(1 << 20, 1 << 20),
        name="finish",
    )(spread, own_block, *blocks)


def on_device(state_ensemble, predicted_data, innovations):
    own = state_ensemble.shape[0] // 8

    def both(chunk):
        return [chunk, sent(chunk, other_core)]

    x0 = pack_data(predicted_data, innovations)
    far = sent(x0, x_far)
    y0 = sent(x0, y_across)
    up = sent(x0, x_up)
    down = sent(x0, x_down)
    state_std, spread = prepare_state(state_ensemble, own)
    y_up = sent(y0, x_up)
    y_down = sent(y0, x_down)
    y_far = sent(far, y_across)
    total = add_chunks(None, state_std, both(x0), "chunks_a")
    total = add_chunks(total, state_std, both(y0) + both(far), "chunks_b")
    total = add_chunks(total, state_std, both(up) + both(down) + both(y_far), "chunks_c")
    blocks = last_chunks(total, state_std, both(y_up) + both(y_down), own)
    arrived = []
    for k in range(1, 8):
        arrived.append(sent(blocks[k], lambda x, y, z, core: (x, y ^ (k // 4), z + k % 4, core)))
    return finish(spread, blocks[0], arrived)


def solution(mesh):
    in_specs = (P("state", None), P(("state", "dp"), None), P(("state", "dp"), None))
    out_specs = P(("state", "dp"), None)
    return jax.shard_map(on_device, mesh=mesh, in_specs=in_specs, out_specs=out_specs, check_vma=False)
```

```python
import jax
import jax.numpy as jnp
from jax import lax
from jax.experimental import pallas as pl
from jax.experimental.pallas import tpu as pltpu
from jax.sharding import PartitionSpec as P


AXES = ("state", "dp")
VMEM = pl.BlockSpec(memory_space=pltpu.VMEM)
HBM = pl.BlockSpec(memory_space=pltpu.HBM)
LIMIT = 24 << 20


def place(i):
    s, d = divmod(i, 8)
    y_hi, rest = divmod(s, 8)
    x, core = divmod(rest, 2)
    y_lo, z = divmod(d, 4)
    return x, y_hi * 2 + y_lo, z, core


def index(x, y, z, core):
    x, y, z = x % 4, y % 4, z % 4
    return ((y // 2) * 8 + x * 2 + core) * 8 + (y % 2) * 4 + z


def sent(value, to):
    return lax.ppermute(value, AXES, [(i, index(*to(*place(i)))) for i in range(128)])


def x_turn(x, y, z, core):
    return x + 1 - 2 * core, y, z, core


def x_back(x, y, z, core):
    return x - 1 + 2 * core, y, z, core


def y_across(x, y, z, core):
    return x, 3 - y, z, core


def other_core(x, y, z, core):
    return x, y, z, 1 - core


def standard(values):
    members = values.shape[1]
    anomalies = values - jnp.mean(values, axis=1, keepdims=True)
    spread = jnp.sqrt(jnp.sum(anomalies * anomalies, axis=1, keepdims=True) / (members - 1) + 1e-06)
    return (anomalies / spread).astype(jnp.bfloat16), spread


def cost(flops, size):
    return pl.CostEstimate(flops=flops, bytes_accessed=size, transcendentals=0)


def pack_data(predicted, innovations):
    rows, members = predicted.shape

    def body(p_hbm, i_hbm, o_ref, p_ref, sems):
        values = pltpu.make_async_copy(p_hbm, p_ref, sems.at[0])
        copied = pltpu.make_async_copy(i_hbm, o_ref.at[:, members:], sems.at[1])
        values.start()
        copied.start()
        values.wait()
        o_ref[:, 0:members] = standard(p_ref[...])[0]
        copied.wait()

    return pl.pallas_call(
        body,
        out_shape=jax.ShapeDtypeStruct((rows, 2 * members), jnp.bfloat16),
        in_specs=[HBM] * 2,
        out_specs=VMEM,
        scratch_shapes=[pltpu.VMEM((rows, members), jnp.float32), pltpu.SemaphoreType.DMA((2,))],
        compiler_params=pltpu.CompilerParams(vmem_limit_bytes=LIMIT),
        cost_estimate=cost(1 << 20, 1 << 20),
        name="pack_data",
    )(predicted, innovations)


def prepare_state(state, own):
    rows, members = state.shape
    count = rows // own

    def body(s_hbm, o_ref, w_ref, s_ref, sems):
        mine = lax.axis_index("dp")
        copies = []
        for i in range(count):
            part = slice(i * own, (i + 1) * own)
            copies.append(pltpu.make_async_copy(s_hbm.at[part, :], s_ref.at[part, :], sems.at[i]))
            copies[i].start()
        for i in range(count):
            part = slice(i * own, (i + 1) * own)
            copies[i].wait()
            std, spread = standard(s_ref[part, :])
            o_ref[part, :] = std

            @pl.when(i == mine)
            def _():
                w_ref[...] = jnp.broadcast_to(spread, (own, members))

    return pl.pallas_call(
        body,
        out_shape=(
            jax.ShapeDtypeStruct((rows, members), jnp.bfloat16),
            jax.ShapeDtypeStruct((own, members), jnp.float32),
        ),
        in_specs=[HBM],
        out_specs=(VMEM, VMEM),
        scratch_shapes=[pltpu.VMEM((rows, members), jnp.float32), pltpu.SemaphoreType.DMA((count,))],
        compiler_params=pltpu.CompilerParams(vmem_limit_bytes=LIMIT),
        cost_estimate=cost(1 << 24, 1 << 22),
        name="prepare_state",
    )(state)


def tile_sum(state, chunks, start, members, width=256):
    total = start
    for chunk in chunks:
        for c in range(0, chunk.shape[0], width):
            correl = lax.dot_general(
                state,
                chunk[c : c + width, 0:members],
                (((1,), (1,)), ((), ())),
                preferred_element_type=jnp.float32,
            ) * (1.0 / (members - 1))
            localized = (correl * correl * correl).astype(jnp.bfloat16)
            part = jnp.dot(localized, chunk[c : c + width, members:], preferred_element_type=jnp.float32)
            total = part if total is None else total + part
    return total


def half_start(far, half):
    lo = lax.axis_index("dp") // 4
    return (1 - lo if far else lo) * half


def add_chunks(parts, chunks, sent_kinds=(), tile=1024):
    members = chunks[0].shape[1] // 2
    half = parts[0][1].shape[0] // 2
    kinds = [jnp.bfloat16 if k in sent_kinds else jnp.float32 for k in range(len(parts))]
    operands, aliases, places = [], {}, []
    for k, (start, state, far) in enumerate(parts):
        if start is not None and kinds[k] == jnp.float32:
            aliases[len(operands)] = k
        if start is not None:
            operands.append(start)
        states = [i for i, o in enumerate(operands) if o is state]
        places.append((None if start is None else len(operands) - 1, len(operands) if not states else states[0], far))
        if not states:
            operands.append(state)
    count = len(operands)
    operands += chunks

    def body(*refs):
        x_refs, o_refs = refs[count : len(operands)], refs[len(operands) :]
        for (start_at, state_at, far), o_ref in zip(places, o_refs):
            base = half_start(far, half)

            def step(i, _):
                there = pl.ds(pl.multiple_of(i * tile, tile), tile)
                part = pl.ds(pl.multiple_of(base + i * tile, tile), tile)
                start = None if start_at is None else refs[start_at][there, :]
                total = tile_sum(refs[state_at][part, :], x_refs, start, members)
                o_ref[there, :] = total.astype(o_ref.dtype)
                return 0

            if tile == half:
                step(0, 0)
            else:
                lax.fori_loop(0, half // tile, step, 0)

    return pl.pallas_call(
        body,
        out_shape=[jax.ShapeDtypeStruct((half, members), kind) for kind in kinds],
        in_specs=[VMEM] * len(operands),
        out_specs=[VMEM] * len(parts),
        input_output_aliases=aliases,
        compiler_params=pltpu.CompilerParams(vmem_limit_bytes=LIMIT),
        cost_estimate=cost(4 * len(parts) * half * members * 512 * len(chunks), 1 << 22),
    )(*operands)


def last_chunks(running, handed, state, chunks, own, far, steps):
    members = running.shape[1]
    count = len(chunks)

    def body(start_ref, handed_ref, s_ref, *refs):
        x_refs, o_refs = refs[:count], refs[count:]
        z = lax.rem(lax.axis_index("dp"), 4)
        base = half_start(far, running.shape[0])
        rows = [pl.multiple_of(lax.rem(z + k, 4) * own, own) for k in steps]
        totals = [start_ref[pl.ds(r, own), :] + handed_ref[pl.ds(r, own), :].astype(jnp.float32) for r in rows]
        if count:
            state_rows = jnp.concatenate([s_ref[pl.ds(base + r, own), :] for r in rows], axis=0)
            total = tile_sum(state_rows, x_refs, jnp.concatenate(totals, axis=0), members)
            totals = [total[j * own : (j + 1) * own, :] for j in range(len(steps))]
        for total, o_ref in zip(totals, o_refs):
            o_ref[...] = total.astype(o_ref.dtype)

    operands = [running, handed, state, *chunks]
    return pl.pallas_call(
        body,
        out_shape=[
            jax.ShapeDtypeStruct((own, members), jnp.bfloat16 if far or k else jnp.float32) for k in steps
        ],
        in_specs=[VMEM] * len(operands),
        out_specs=[VMEM] * len(steps),
        compiler_params=pltpu.CompilerParams(vmem_limit_bytes=LIMIT),
        cost_estimate=cost(4 * len(steps) * own * members * 512 * count + (1 << 20), 1 << 22),
    )(*operands)


def finish(spread, own_block, blocks):
    def body(w_ref, f_ref, *refs):
        total = f_ref[...]
        for ref in refs[:-1]:
            total = total + ref[...].astype(jnp.float32)
        refs[-1][...] = w_ref[...] * total

    return pl.pallas_call(
        body,
        out_shape=jax.ShapeDtypeStruct(own_block.shape, jnp.float32),
        in_specs=[VMEM] * (2 + len(blocks)),
        out_specs=VMEM,
        compiler_params=pltpu.CompilerParams(vmem_limit_bytes=LIMIT),
        cost_estimate=cost(1 << 20, 1 << 20),
        name="finish",
    )(spread, own_block, *blocks)


def update(state_ensemble, predicted_data, innovations):
    own = state_ensemble.shape[0] // 8
    x0 = pack_data(predicted_data, innovations)
    p1a = sent(x0, x_turn)
    y0 = sent(x0, y_across)
    s, spread = prepare_state(state_ensemble, own)
    t = sent(s, other_core)
    p1b = sent(x0, x_back)
    p2 = sent(p1a, x_turn)
    q1a = sent(y0, x_turn)
    q1b = sent(y0, x_back)
    y2 = sent(p2, y_across)
    early = [(None, s, True), (None, t, True), (None, s, False), (None, t, False)]
    fs, ft, ns, nt = add_chunks(early, [x0, p1a])
    ns, nt = add_chunks([(ns, s, False), (nt, t, False)], [p1b, y0])
    fs, ft = add_chunks([(fs, s, True), (ft, t, True)], [p1b, y0])
    fs, ft = add_chunks([(fs, s, True), (ft, t, True)], [p2, q1a])
    ns, nt = add_chunks([(ns, s, False), (nt, t, False)], [p2, q1a])
    fs, ft = add_chunks([(fs, s, True), (ft, t, True)], [q1b], sent_kinds=(1,))
    fh = sent(ft, other_core)
    ns, nt = add_chunks([(ns, s, False), (nt, t, False)], [q1b], sent_kinds=(1,))
    nh = sent(nt, other_core)
    y2s = sent(y2, other_core)
    (fs,) = add_chunks([(fs, s, True)], [y2])
    blocks = {}
    blocks[1, 2], blocks[1, 1] = last_chunks(fs, fh, s, [y2s], own, True, (2, 1))
    blocks[1, 3], blocks[1, 0] = last_chunks(fs, fh, s, [y2s], own, True, (3, 0))
    near = last_chunks(ns, nh, s, [y2, y2s], own, False, (1, 3, 2, 0))
    blocks[0, 1], blocks[0, 3], blocks[0, 2], mine = near
    arrived = []
    for (across, k), block in blocks.items():
        arrived.append(sent(block, lambda x, y, z, core: (x, y ^ across, z + k, core)))
    return finish(spread, mine, arrived)


def solution(mesh):
    in_specs = (P("state", None), P(("state", "dp"), None), P(("state", "dp"), None))
    out_specs = P(("state", "dp"), None)
    return jax.shard_map(update, mesh=mesh, in_specs=in_specs, out_specs=out_specs, check_vma=False)
```

```python
import jax
import jax.numpy as jnp
from jax import lax
from jax.experimental import pallas as pl
from jax.experimental.pallas import tpu as pltpu
from jax.sharding import PartitionSpec as P


AXES = ("state", "dp")
VMEM = pl.BlockSpec(memory_space=pltpu.VMEM)
HBM = pl.BlockSpec(memory_space=pltpu.HBM)
LIMIT = 24 << 20


def place(i):
    s, d = divmod(i, 8)
    y_hi, rest = divmod(s, 8)
    x, core = divmod(rest, 2)
    y_lo, z = divmod(d, 4)
    return x, y_hi * 2 + y_lo, z, core


def index(x, y, z, core):
    x, y, z = x % 4, y % 4, z % 4
    return ((y // 2) * 8 + x * 2 + core) * 8 + (y % 2) * 4 + z


def sent(value, to):
    return lax.ppermute(value, AXES, [(i, index(*to(*place(i)))) for i in range(128)])


def x_turn(x, y, z, core):
    return x + 1 - 2 * core, y, z, core


def x_back(x, y, z, core):
    return x - 1 + 2 * core, y, z, core


def y_across(x, y, z, core):
    return x, 3 - y, z, core


def other_core(x, y, z, core):
    return x, y, z, 1 - core


def standard(values):
    members = values.shape[1]
    anomalies = values - jnp.mean(values, axis=1, keepdims=True)
    spread = jnp.sqrt(jnp.sum(anomalies * anomalies, axis=1, keepdims=True) / (members - 1) + 1e-06)
    return (anomalies / spread).astype(jnp.bfloat16), spread


def cost(flops, size):
    return pl.CostEstimate(flops=flops, bytes_accessed=size, transcendentals=0)


def pack_data(predicted, innovations):
    rows, members = predicted.shape
    pieces = 4
    step = rows // pieces

    def body(p_hbm, i_hbm, o_ref, p_ref, i_ref, sems):
        copies = []
        for k in range(pieces):
            part = pl.ds(k * step, step)
            copies.append(pltpu.make_async_copy(p_hbm.at[part, :], p_ref.at[part, :], sems.at[k]))
        copies.append(pltpu.make_async_copy(i_hbm, i_ref, sems.at[pieces]))
        for copy in copies:
            copy.start()
        for k in range(pieces):
            copies[k].wait()
            part = pl.ds(k * step, step)
            o_ref[part, 0:members] = standard(p_ref[part, :])[0]
        copies[pieces].wait()
        o_ref[:, members:] = i_ref[...]

    return pl.pallas_call(
        body,
        out_shape=jax.ShapeDtypeStruct((rows, 2 * members), jnp.bfloat16),
        in_specs=[HBM] * 2,
        out_specs=VMEM,
        scratch_shapes=[
            pltpu.VMEM((rows, members), jnp.float32),
            pltpu.VMEM((rows, members), jnp.bfloat16),
            pltpu.SemaphoreType.DMA((pieces + 1,)),
        ],
        compiler_params=pltpu.CompilerParams(vmem_limit_bytes=LIMIT),
        cost_estimate=cost(1 << 20, 1 << 20),
        name="pack_data",
    )(
        pltpu.with_memory_space_constraint(predicted, pltpu.HBM),
        pltpu.with_memory_space_constraint(innovations, pltpu.HBM),
    )


def prepare_state(state, own):
    rows, members = state.shape
    count = rows // own

    def body(s_hbm, o_ref, w_ref, s_ref, sems):
        mine = lax.axis_index("dp")
        copies = []
        for i in range(count):
            part = slice(i * own, (i + 1) * own)
            copies.append(pltpu.make_async_copy(s_hbm.at[part, :], s_ref.at[part, :], sems.at[i]))
            copies[i].start()
        for i in range(count):
            part = slice(i * own, (i + 1) * own)
            copies[i].wait()
            std, spread = standard(s_ref[part, :])
            o_ref[part, :] = std

            @pl.when(i == mine)
            def _():
                w_ref[...] = jnp.broadcast_to(spread, (own, members))

    return pl.pallas_call(
        body,
        out_shape=(
            jax.ShapeDtypeStruct((rows, members), jnp.bfloat16),
            jax.ShapeDtypeStruct((own, members), jnp.float32),
        ),
        in_specs=[HBM],
        out_specs=(VMEM, VMEM),
        scratch_shapes=[pltpu.VMEM((rows, members), jnp.float32), pltpu.SemaphoreType.DMA((count,))],
        compiler_params=pltpu.CompilerParams(vmem_limit_bytes=LIMIT),
        cost_estimate=cost(1 << 24, 1 << 22),
        name="prepare_state",
    )(state)


def tile_sum(state, chunks, start, members, width=256):
    total = start
    for chunk in chunks:
        for c in range(0, chunk.shape[0], width):
            correl = lax.dot_general(
                state,
                chunk[c : c + width, 0:members],
                (((1,), (1,)), ((), ())),
                preferred_element_type=jnp.float32,
            ) * (1.0 / (members - 1))
            localized = (correl * correl * correl).astype(jnp.bfloat16)
            part = jnp.dot(localized, chunk[c : c + width, members:], preferred_element_type=jnp.float32)
            total = part if total is None else total + part
    return total


def half_start(first, mine, half):
    core = lax.rem(lax.axis_index("state"), 2)
    lo = lax.axis_index("dp") // 4
    return lax.rem(lo + core + (1 if first == mine else 0), 2) * half


def add_chunks(parts, chunks, sent_kinds=(), tile=1024):
    members = chunks[0].shape[1] // 2
    half = parts[0][1].shape[0] // 2
    kinds = [jnp.bfloat16 if k in sent_kinds else jnp.float32 for k in range(len(parts))]
    operands, aliases, places = [], {}, []
    for k, (start, state, *which) in enumerate(parts):
        if start is not None and kinds[k] == jnp.float32:
            aliases[len(operands)] = k
        if start is not None:
            operands.append(start)
        states = [i for i, o in enumerate(operands) if o is state]
        places.append((None if start is None else len(operands) - 1, len(operands) if not states else states[0], which))
        if not states:
            operands.append(state)
    count = len(operands)
    operands += chunks

    def body(*refs):
        x_refs, o_refs = refs[count : len(operands)], refs[len(operands) :]
        for (start_at, state_at, which), o_ref in zip(places, o_refs):
            base = half_start(*which, half)

            def step(i, _):
                there = pl.ds(pl.multiple_of(i * tile, tile), tile)
                part = pl.ds(pl.multiple_of(base + i * tile, tile), tile)
                start = None if start_at is None else refs[start_at][there, :]
                total = tile_sum(refs[state_at][part, :], x_refs, start, members)
                o_ref[there, :] = total.astype(o_ref.dtype)
                return 0

            if tile == half:
                step(0, 0)
            else:
                lax.fori_loop(0, half // tile, step, 0)

    return pl.pallas_call(
        body,
        out_shape=[jax.ShapeDtypeStruct((half, members), kind) for kind in kinds],
        in_specs=[VMEM] * len(operands),
        out_specs=[VMEM] * len(parts),
        input_output_aliases=aliases,
        compiler_params=pltpu.CompilerParams(vmem_limit_bytes=LIMIT),
        cost_estimate=cost(4 * len(parts) * half * members * 512 * len(chunks), 1 << 22),
    )(*operands)


def last_chunks(running, handed, state, chunks, own, first, steps, kept=None):
    members = running.shape[1]
    count = len(chunks)

    def body(start_ref, handed_ref, s_ref, *refs):
        x_refs, o_refs = refs[:count], refs[count + (kept is not None) :]
        z = lax.rem(lax.axis_index("dp"), 4)
        base = half_start(first, True, running.shape[0])
        rows = [pl.multiple_of(lax.rem(z + k, 4) * own, own) for k in steps]
        totals = [start_ref[pl.ds(r, own), :] + handed_ref[pl.ds(r, own), :].astype(jnp.float32) for r in rows]
        state_rows = jnp.concatenate([s_ref[pl.ds(base + r, own), :] for r in rows], axis=0)
        total = tile_sum(state_rows, x_refs, jnp.concatenate(totals, axis=0), members)
        blocks = [total[j * own : (j + 1) * own, :] for j in range(len(steps))]
        if kept is not None:
            upper = jnp.full(blocks[-1].shape, lax.rem(lax.axis_index("state"), 2)) == 1
            mine, other = blocks[-1], refs[count][...]
            blocks[-1:] = [jnp.where(upper, mine, other), jnp.where(upper, other, mine)]
        for block, o_ref in zip(blocks, o_refs):
            o_ref[...] = block.astype(o_ref.dtype)

    operands = [running, handed, state, *chunks] + ([] if kept is None else [kept])
    kinds = [jnp.float32 if k == 0 and kept is None else jnp.bfloat16 for k in steps]
    kinds += [] if kept is None else [jnp.float32]
    return pl.pallas_call(
        body,
        out_shape=[jax.ShapeDtypeStruct((own, members), kind) for kind in kinds],
        in_specs=[VMEM] * len(operands),
        out_specs=[VMEM] * len(kinds),
        compiler_params=pltpu.CompilerParams(vmem_limit_bytes=LIMIT),
        cost_estimate=cost(4 * len(steps) * own * members * 512 * count + (1 << 20), 1 << 22),
    )(*operands)


def finish(spread, blocks):
    def body(w_ref, *refs):
        total = refs[0][...].astype(jnp.float32)
        for ref in refs[1:-1]:
            total = total + ref[...].astype(jnp.float32)
        refs[-1][...] = w_ref[...] * total

    return pl.pallas_call(
        body,
        out_shape=jax.ShapeDtypeStruct(spread.shape, jnp.float32),
        in_specs=[VMEM] * (1 + len(blocks)),
        out_specs=VMEM,
        compiler_params=pltpu.CompilerParams(vmem_limit_bytes=LIMIT),
        cost_estimate=cost(1 << 20, 1 << 20),
        name="finish",
    )(spread, *blocks)


def update(state_ensemble, predicted_data, innovations):
    own = state_ensemble.shape[0] // 8
    x0 = pack_data(predicted_data, innovations)
    p1a = sent(x0, x_turn)
    y0 = sent(x0, y_across)
    s, spread = prepare_state(state_ensemble, own)
    t = sent(s, other_core)
    p1b = sent(x0, x_back)
    p2 = sent(p1a, x_turn)
    q1a = sent(y0, x_turn)
    q1b = sent(y0, x_back)
    y2 = sent(p2, y_across)

    def added(sums, chunks):
        rows = ((s, True, True), (t, True, False), (s, False, True), (t, False, False))
        return add_chunks([(total, *row) for total, row in zip(sums, rows)], chunks)

    sums = added([None] * 4, [x0, p1a])
    sums = added(sums, [y0])
    sums = added(sums, [p1b, p2])
    fs, ft, ns, nt = added(sums, [q1a])
    fs, ft = add_chunks([(fs, s, True, True), (ft, t, True, False)], [q1b], sent_kinds=(1,))
    fh = sent(ft, other_core)
    ns, nt = add_chunks([(ns, s, False, True), (nt, t, False, False)], [q1b], sent_kinds=(1,))
    nh = sent(nt, other_core)
    y2s = sent(y2, other_core)
    (fs,) = add_chunks([(fs, s, True, True)], [y2])
    blocks = {}
    blocks[0, 2], blocks[0, 1] = last_chunks(fs, fh, s, [y2s], own, True, (2, 1))
    blocks[0, 3], kept = last_chunks(fs, fh, s, [y2s], own, True, (3, 0))
    second = last_chunks(ns, nh, s, [y2, y2s], own, False, (2, 1, 3, 0), kept)
    blocks[1, 2], blocks[1, 1], blocks[1, 3], across, mine = second
    arrived = [mine, sent(across, lambda x, y, z, core: (x, y ^ 1, z, core))]
    for (later, k), block in blocks.items():
        arrived.append(sent(block, lambda x, y, z, core: (x, y ^ int(core == later), z + k, core)))
    return finish(spread, arrived)


def solution(mesh):
    in_specs = (P("state", None), P(("state", "dp"), None), P(("state", "dp"), None))
    out_specs = P(("state", "dp"), None)
    return jax.shard_map(update, mesh=mesh, in_specs=in_specs, out_specs=out_specs, check_vma=False)
```

```python
import jax
import jax.numpy as jnp
from jax import lax
from jax.experimental import pallas as pl
from jax.experimental.pallas import tpu as pltpu
from jax.sharding import PartitionSpec as P


AXES = ("state", "dp")
VMEM = pl.BlockSpec(memory_space=pltpu.VMEM)
HBM = pl.BlockSpec(memory_space=pltpu.HBM)
LIMIT = 24 << 20


def place(i):
    s, d = divmod(i, 8)
    y_hi, rest = divmod(s, 8)
    x, core = divmod(rest, 2)
    y_lo, z = divmod(d, 4)
    return x, y_hi * 2 + y_lo, z, core


def index(x, y, z, core):
    x, y, z = x % 4, y % 4, z % 4
    return ((y // 2) * 8 + x * 2 + core) * 8 + (y % 2) * 4 + z


def sent(value, to):
    return lax.ppermute(value, AXES, [(i, index(*to(*place(i)))) for i in range(128)])


def x_turn(x, y, z, core):
    return x + 1 - 2 * core, y, z, core


def x_back(x, y, z, core):
    return x - 1 + 2 * core, y, z, core


def y_across(x, y, z, core):
    return x, 3 - y, z, core


def other_core(x, y, z, core):
    return x, y, z, 1 - core


def standard(values):
    members = values.shape[1]
    anomalies = values - jnp.mean(values, axis=1, keepdims=True)
    spread = jnp.sqrt(jnp.sum(anomalies * anomalies, axis=1, keepdims=True) / (members - 1) + 1e-06)
    return (anomalies / spread).astype(jnp.bfloat16), spread


def cost(flops, size):
    return pl.CostEstimate(flops=flops, bytes_accessed=size, transcendentals=0)


def pack_data(predicted, innovations):
    rows, members = predicted.shape
    pieces = 4
    step = rows // pieces

    def body(p_hbm, i_hbm, o_ref, p_ref, i_ref, sems):
        copies = []
        for k in range(pieces):
            part = pl.ds(k * step, step)
            copies.append(pltpu.make_async_copy(p_hbm.at[part, :], p_ref.at[part, :], sems.at[k]))
        copies.append(pltpu.make_async_copy(i_hbm, i_ref, sems.at[pieces]))
        for copy in copies:
            copy.start()
        for k in range(pieces):
            copies[k].wait()
            part = pl.ds(k * step, step)
            o_ref[part, 0:members] = standard(p_ref[part, :])[0]
        copies[pieces].wait()
        o_ref[:, members:] = i_ref[...]

    return pl.pallas_call(
        body,
        out_shape=jax.ShapeDtypeStruct((rows, 2 * members), jnp.bfloat16),
        in_specs=[HBM] * 2,
        out_specs=VMEM,
        scratch_shapes=[
            pltpu.VMEM((rows, members), jnp.float32),
            pltpu.VMEM((rows, members), jnp.bfloat16),
            pltpu.SemaphoreType.DMA((pieces + 1,)),
        ],
        compiler_params=pltpu.CompilerParams(vmem_limit_bytes=LIMIT),
        cost_estimate=cost(1 << 20, 1 << 20),
        name="pack_data",
    )(
        pltpu.with_memory_space_constraint(predicted, pltpu.HBM),
        pltpu.with_memory_space_constraint(innovations, pltpu.HBM),
    )


def prepare_state(state, own):
    rows, members = state.shape
    count = rows // own

    def body(s_hbm, o_ref, w_ref, s_ref, sems):
        mine = lax.axis_index("dp")
        copies = []
        for i in range(count):
            part = slice(i * own, (i + 1) * own)
            copies.append(pltpu.make_async_copy(s_hbm.at[part, :], s_ref.at[part, :], sems.at[i]))
            copies[i].start()
        for i in range(count):
            part = slice(i * own, (i + 1) * own)
            copies[i].wait()
            std, spread = standard(s_ref[part, :])
            o_ref[part, :] = std

            @pl.when(i == mine)
            def _():
                w_ref[...] = jnp.broadcast_to(spread, (own, members))

    return pl.pallas_call(
        body,
        out_shape=(
            jax.ShapeDtypeStruct((rows, members), jnp.bfloat16),
            jax.ShapeDtypeStruct((own, members), jnp.float32),
        ),
        in_specs=[HBM],
        out_specs=(VMEM, VMEM),
        scratch_shapes=[pltpu.VMEM((rows, members), jnp.float32), pltpu.SemaphoreType.DMA((count,))],
        compiler_params=pltpu.CompilerParams(vmem_limit_bytes=LIMIT),
        cost_estimate=cost(1 << 24, 1 << 22),
        name="prepare_state",
    )(state)


def correlations(state, chunk, members):
    return lax.dot_general(
        state, chunk[:, 0:members], (((1,), (1,)), ((), ())), preferred_element_type=jnp.float32
    ) * (1.0 / (members - 1))


def tile_sums(states, starts, chunks, members):
    steps = [(tile, chunk) for tile in range(len(states)) for chunk in range(len(chunks))]
    totals = list(starts)
    ahead = None
    for n, (tile, chunk) in enumerate(steps):
        correl = correlations(states[tile](), chunks[chunk][...], members) if ahead is None else ahead
        ahead = None
        if n + 1 < len(steps):
            ahead = correlations(states[steps[n + 1][0]](), chunks[steps[n + 1][1]][...], members)
        localized = (correl * correl * correl).astype(jnp.bfloat16)
        part = jnp.dot(localized, chunks[chunk][:, members:], preferred_element_type=jnp.float32)
        start = totals[tile]() if chunk == 0 and totals[tile] is not None else totals[tile]
        totals[tile] = part if start is None else start + part
        if chunk == len(chunks) - 1:
            yield totals[tile]


def half_start(first, mine, half):
    core = lax.rem(lax.axis_index("state"), 2)
    lo = lax.axis_index("dp") // 4
    return lax.rem(lo + core + (1 if first == mine else 0), 2) * half


def add_chunks(parts, chunks, sent_kinds=()):
    members = chunks[0].shape[1] // 2
    half = parts[0][1].shape[0] // 2
    kinds = [jnp.bfloat16 if k in sent_kinds else jnp.float32 for k in range(len(parts))]
    operands, aliases, places = [], {}, []
    for k, (start, state, *which) in enumerate(parts):
        if start is not None and kinds[k] == jnp.float32:
            aliases[len(operands)] = k
        if start is not None:
            operands.append(start)
        states = [i for i, o in enumerate(operands) if o is state]
        places.append((None if start is None else len(operands) - 1, len(operands) if not states else states[0], which))
        if not states:
            operands.append(state)
    count = len(operands)
    operands += chunks

    def body(*refs):
        x_refs, o_refs = refs[count : len(operands)], refs[len(operands) :]
        states, starts = [], []
        for start_at, state_at, which in places:
            base = pl.multiple_of(half_start(*which, half), half)
            states.append(lambda at=state_at, base=base: refs[at][pl.ds(base, half), :])
            starts.append(None if start_at is None else lambda at=start_at: refs[at][...])
        for total, o_ref in zip(tile_sums(states, starts, x_refs, members), o_refs):
            o_ref[...] = total.astype(o_ref.dtype)

    return pl.pallas_call(
        body,
        out_shape=[jax.ShapeDtypeStruct((half, members), kind) for kind in kinds],
        in_specs=[VMEM] * len(operands),
        out_specs=[VMEM] * len(parts),
        input_output_aliases=aliases,
        compiler_params=pltpu.CompilerParams(vmem_limit_bytes=LIMIT),
        cost_estimate=cost(4 * len(parts) * half * members * 512 * len(chunks), 1 << 22),
    )(*operands)


def last_chunks(running, handed, state, chunks, own, first, steps, kept=None):
    members = running.shape[1]
    count = len(chunks)

    def body(start_ref, handed_ref, s_ref, *refs):
        x_refs, o_refs = refs[:count], refs[count + (kept is not None) :]
        z = lax.rem(lax.axis_index("dp"), 4)
        base = half_start(first, True, running.shape[0])
        rows = [pl.multiple_of(lax.rem(z + k, 4) * own, own) for k in steps]
        totals = [start_ref[pl.ds(r, own), :] + handed_ref[pl.ds(r, own), :].astype(jnp.float32) for r in rows]
        state_rows = jnp.concatenate([s_ref[pl.ds(base + r, own), :] for r in rows], axis=0)
        start = jnp.concatenate(totals, axis=0)
        (total,) = tile_sums([lambda: state_rows], [lambda: start], x_refs, members)
        blocks = [total[j * own : (j + 1) * own, :] for j in range(len(steps))]
        if kept is not None:
            upper = jnp.full(blocks[-1].shape, lax.rem(lax.axis_index("state"), 2)) == 1
            mine, other = blocks[-1], refs[count][...]
            blocks[-1:] = [jnp.where(upper, mine, other), jnp.where(upper, other, mine)]
        for block, o_ref in zip(blocks, o_refs):
            o_ref[...] = block.astype(o_ref.dtype)

    operands = [running, handed, state, *chunks] + ([] if kept is None else [kept])
    kinds = [jnp.float32 if k == 0 and kept is None else jnp.bfloat16 for k in steps]
    kinds += [] if kept is None else [jnp.float32]
    return pl.pallas_call(
        body,
        out_shape=[jax.ShapeDtypeStruct((own, members), kind) for kind in kinds],
        in_specs=[VMEM] * len(operands),
        out_specs=[VMEM] * len(kinds),
        compiler_params=pltpu.CompilerParams(vmem_limit_bytes=LIMIT),
        cost_estimate=cost(4 * len(steps) * own * members * 512 * count + (1 << 20), 1 << 22),
    )(*operands)


def finish(spread, blocks):
    def body(w_ref, *refs):
        total = refs[0][...].astype(jnp.float32)
        for ref in refs[1:-1]:
            total = total + ref[...].astype(jnp.float32)
        refs[-1][...] = w_ref[...] * total

    return pl.pallas_call(
        body,
        out_shape=jax.ShapeDtypeStruct(spread.shape, jnp.float32),
        in_specs=[VMEM] * (1 + len(blocks)),
        out_specs=VMEM,
        compiler_params=pltpu.CompilerParams(vmem_limit_bytes=LIMIT),
        cost_estimate=cost(1 << 20, 1 << 20),
        name="finish",
    )(spread, *blocks)


def update(state_ensemble, predicted_data, innovations):
    own = state_ensemble.shape[0] // 8
    x0 = pack_data(predicted_data, innovations)
    p1a = sent(x0, x_turn)
    y0 = sent(x0, y_across)
    s, spread = prepare_state(state_ensemble, own)
    t = sent(s, other_core)
    p1b = sent(x0, x_back)
    p2 = sent(p1a, x_turn)
    q1a = sent(y0, x_turn)
    q1b = sent(y0, x_back)
    y2 = sent(p2, y_across)

    def added(sums, chunks):
        rows = ((s, True, True), (t, True, False), (s, False, True), (t, False, False))
        return add_chunks([(total, *row) for total, row in zip(sums, rows)], chunks)

    sums = added([None] * 4, [x0, p1a])
    sums = added(sums, [y0])
    sums = added(sums, [p1b, p2])
    fs, ft, ns, nt = added(sums, [q1a])
    fs, ft = add_chunks([(fs, s, True, True), (ft, t, True, False)], [q1b], sent_kinds=(1,))
    fh = sent(ft, other_core)
    ns, nt = add_chunks([(ns, s, False, True), (nt, t, False, False)], [q1b], sent_kinds=(1,))
    nh = sent(nt, other_core)
    y2s = sent(y2, other_core)
    (fs,) = add_chunks([(fs, s, True, True)], [y2])
    blocks = {}
    blocks[0, 1], blocks[0, 3] = last_chunks(fs, fh, s, [y2s], own, True, (1, 3))
    blocks[0, 2], kept = last_chunks(fs, fh, s, [y2s], own, True, (2, 0))
    second = last_chunks(ns, nh, s, [y2, y2s], own, False, (2, 1, 3, 0), kept)
    blocks[1, 2], blocks[1, 1], blocks[1, 3], across, mine = second
    arrived = [mine, sent(across, lambda x, y, z, core: (x, y ^ 1, z, core))]
    for (later, k), block in blocks.items():
        arrived.append(sent(block, lambda x, y, z, core: (x, y ^ int(core == later), z + k, core)))
    return finish(spread, arrived)


def solution(mesh):
    in_specs = (P("state", None), P(("state", "dp"), None), P(("state", "dp"), None))
    out_specs = P(("state", "dp"), None)
    return jax.shard_map(update, mesh=mesh, in_specs=in_specs, out_specs=out_specs, check_vma=False)
```

```python
import jax
import jax.numpy as jnp
from jax import lax
from jax.experimental import pallas as pl
from jax.experimental.pallas import tpu as pltpu
from jax.sharding import PartitionSpec as P


AXES = ("state", "dp")
VMEM = pl.BlockSpec(memory_space=pltpu.VMEM)
HBM = pl.BlockSpec(memory_space=pltpu.HBM)
LIMIT = 24 << 20


def place(i):
    s, d = divmod(i, 8)
    y_hi, rest = divmod(s, 8)
    x, core = divmod(rest, 2)
    y_lo, z = divmod(d, 4)
    return x, y_hi * 2 + y_lo, z, core


def index(x, y, z, core):
    x, y, z = x % 4, y % 4, z % 4
    return ((y // 2) * 8 + x * 2 + core) * 8 + (y % 2) * 4 + z


def sent(value, to):
    return lax.ppermute(value, AXES, [(i, index(*to(*place(i)))) for i in range(128)])


def x_turn(x, y, z, core):
    return x + 1 - 2 * core, y, z, core


def x_back(x, y, z, core):
    return x - 1 + 2 * core, y, z, core


def y_across(x, y, z, core):
    return x, 3 - y, z, core


def other_core(x, y, z, core):
    return x, y, z, 1 - core


def standard(values):
    members = values.shape[1]
    anomalies = values - jnp.mean(values, axis=1, keepdims=True)
    spread = jnp.sqrt(jnp.sum(anomalies * anomalies, axis=1, keepdims=True) / (members - 1) + 1e-06)
    return (anomalies / spread).astype(jnp.bfloat16), spread


def cost(flops, size):
    return pl.CostEstimate(flops=flops, bytes_accessed=size, transcendentals=0)


def pack_data(predicted, innovations):
    rows, members = predicted.shape
    pieces = 4
    step = rows // pieces

    def body(p_hbm, i_hbm, o_ref, p_ref, i_ref, sems):
        copies = []
        for k in range(pieces):
            part = pl.ds(k * step, step)
            copies.append(pltpu.make_async_copy(p_hbm.at[part, :], p_ref.at[part, :], sems.at[k]))
        copies.append(pltpu.make_async_copy(i_hbm, i_ref, sems.at[pieces]))
        for copy in copies:
            copy.start()
        for k in range(pieces):
            copies[k].wait()
            part = pl.ds(k * step, step)
            o_ref[part, 0:members] = standard(p_ref[part, :])[0]
        copies[pieces].wait()
        o_ref[:, members:] = i_ref[...]

    return pl.pallas_call(
        body,
        out_shape=jax.ShapeDtypeStruct((rows, 2 * members), jnp.bfloat16),
        in_specs=[HBM] * 2,
        out_specs=VMEM,
        scratch_shapes=[
            pltpu.VMEM((rows, members), jnp.float32),
            pltpu.VMEM((rows, members), jnp.bfloat16),
            pltpu.SemaphoreType.DMA((pieces + 1,)),
        ],
        compiler_params=pltpu.CompilerParams(vmem_limit_bytes=LIMIT),
        cost_estimate=cost(1 << 20, 1 << 20),
        name="pack_data",
    )(
        pltpu.with_memory_space_constraint(predicted, pltpu.HBM),
        pltpu.with_memory_space_constraint(innovations, pltpu.HBM),
    )


def prepare_state(state, own):
    rows, members = state.shape
    count = rows // own

    def body(s_hbm, o_ref, w_ref, s_ref, sems):
        mine = lax.axis_index("dp")
        copies = []
        for i in range(count):
            part = slice(i * own, (i + 1) * own)
            copies.append(pltpu.make_async_copy(s_hbm.at[part, :], s_ref.at[part, :], sems.at[i]))
            copies[i].start()
        for i in range(count):
            part = slice(i * own, (i + 1) * own)
            copies[i].wait()
            std, spread = standard(s_ref[part, :])
            o_ref[part, :] = std

            @pl.when(i == mine)
            def _():
                w_ref[...] = jnp.broadcast_to(spread, (own, members))

    return pl.pallas_call(
        body,
        out_shape=(
            jax.ShapeDtypeStruct((rows, members), jnp.bfloat16),
            jax.ShapeDtypeStruct((own, members), jnp.float32),
        ),
        in_specs=[HBM],
        out_specs=(VMEM, VMEM),
        scratch_shapes=[pltpu.VMEM((rows, members), jnp.float32), pltpu.SemaphoreType.DMA((count,))],
        compiler_params=pltpu.CompilerParams(vmem_limit_bytes=LIMIT),
        cost_estimate=cost(1 << 24, 1 << 22),
        name="prepare_state",
    )(state)


def correlations(state, chunk, members):
    return lax.dot_general(
        state, chunk[:, 0:members], (((1,), (1,)), ((), ())), preferred_element_type=jnp.float32
    ) * (1.0 / (members - 1))


def tile_sums(states, starts, chunks, members):
    steps = [(tile, chunk) for tile in range(len(states)) for chunk in range(len(chunks))]
    totals = list(starts)
    ahead = None
    for n, (tile, chunk) in enumerate(steps):
        correl = correlations(states[tile](), chunks[chunk][...], members) if ahead is None else ahead
        ahead = None
        if n + 1 < len(steps):
            ahead = correlations(states[steps[n + 1][0]](), chunks[steps[n + 1][1]][...], members)
        localized = (correl * correl * correl).astype(jnp.bfloat16)
        part = jnp.dot(localized, chunks[chunk][:, members:], preferred_element_type=jnp.float32)
        start = totals[tile]() if chunk == 0 and totals[tile] is not None else totals[tile]
        totals[tile] = part if start is None else start + part
        if chunk == len(chunks) - 1:
            yield totals[tile]


def half_start(first, mine, half):
    core = lax.rem(lax.axis_index("state"), 2)
    lo = lax.axis_index("dp") // 4
    return lax.rem(lo + core + (1 if first == mine else 0), 2) * half


def add_chunks(parts, chunks, sent_kinds=()):
    members = chunks[0].shape[1] // 2
    half = parts[0][1].shape[0] // 2
    kinds = [jnp.bfloat16 if k in sent_kinds else jnp.float32 for k in range(len(parts))]
    operands, aliases, places = [], {}, []
    for k, (start, state, *which) in enumerate(parts):
        if start is not None and kinds[k] == jnp.float32:
            aliases[len(operands)] = k
        if start is not None:
            operands.append(start)
        states = [i for i, o in enumerate(operands) if o is state]
        places.append((None if start is None else len(operands) - 1, len(operands) if not states else states[0], which))
        if not states:
            operands.append(state)
    count = len(operands)
    operands += chunks

    def body(*refs):
        x_refs, o_refs = refs[count : len(operands)], refs[len(operands) :]
        states, starts = [], []
        for start_at, state_at, which in places:
            base = pl.multiple_of(half_start(*which, half), half)
            states.append(lambda at=state_at, base=base: refs[at][pl.ds(base, half), :])
            starts.append(None if start_at is None else lambda at=start_at: refs[at][...])
        for total, o_ref in zip(tile_sums(states, starts, x_refs, members), o_refs):
            o_ref[...] = total.astype(o_ref.dtype)

    return pl.pallas_call(
        body,
        out_shape=[jax.ShapeDtypeStruct((half, members), kind) for kind in kinds],
        in_specs=[VMEM] * len(operands),
        out_specs=[VMEM] * len(parts),
        input_output_aliases=aliases,
        compiler_params=pltpu.CompilerParams(vmem_limit_bytes=LIMIT),
        cost_estimate=cost(4 * len(parts) * half * members * 512 * len(chunks), 1 << 22),
    )(*operands)


def last_chunks(running, handed, state, chunks, own, first, steps, kept=None):
    members = running.shape[1]
    count = len(chunks)

    def body(start_ref, handed_ref, s_ref, *refs):
        x_refs, o_refs = refs[:count], refs[count + (kept is not None) :]
        z = lax.rem(lax.axis_index("dp"), 4)
        base = half_start(first, True, running.shape[0])
        rows = [pl.multiple_of(lax.rem(z + k, 4) * own, own) for k in steps]
        totals = [start_ref[pl.ds(r, own), :] + handed_ref[pl.ds(r, own), :].astype(jnp.float32) for r in rows]
        state_rows = jnp.concatenate([s_ref[pl.ds(base + r, own), :] for r in rows], axis=0)
        start = jnp.concatenate(totals, axis=0)
        (total,) = tile_sums([lambda: state_rows], [lambda: start], x_refs, members)
        blocks = [total[j * own : (j + 1) * own, :] for j in range(len(steps))]
        if kept is not None:
            upper = jnp.full(blocks[-1].shape, lax.rem(lax.axis_index("state"), 2)) == 1
            mine, other = blocks[-1], refs[count][...]
            blocks[-1:] = [jnp.where(upper, mine, other), jnp.where(upper, other, mine)]
        for block, o_ref in zip(blocks, o_refs):
            o_ref[...] = block.astype(o_ref.dtype)

    operands = [running, handed, state, *chunks] + ([] if kept is None else [kept])
    kinds = [jnp.float32 if k == 0 and kept is None else jnp.bfloat16 for k in steps]
    kinds += [] if kept is None else [jnp.float32]
    return pl.pallas_call(
        body,
        out_shape=[jax.ShapeDtypeStruct((own, members), kind) for kind in kinds],
        in_specs=[VMEM] * len(operands),
        out_specs=[VMEM] * len(kinds),
        compiler_params=pltpu.CompilerParams(vmem_limit_bytes=LIMIT),
        cost_estimate=cost(4 * len(steps) * own * members * 512 * count + (1 << 20), 1 << 22),
    )(*operands)


def early_sum(blocks):
    def body(*refs):
        total = refs[0][...].astype(jnp.float32)
        for ref in refs[1:-1]:
            total = total + ref[...].astype(jnp.float32)
        refs[-1][...] = total

    return pl.pallas_call(
        body,
        out_shape=jax.ShapeDtypeStruct(blocks[0].shape, jnp.float32),
        in_specs=[VMEM] * len(blocks),
        out_specs=VMEM,
        compiler_params=pltpu.CompilerParams(vmem_limit_bytes=LIMIT),
        cost_estimate=cost(1 << 20, 1 << 20),
        name="early_sum",
    )(*blocks)


def finish(spread, blocks):
    def body(w_ref, *refs):
        total = refs[0][...].astype(jnp.float32)
        for ref in refs[1:-1]:
            total = total + ref[...].astype(jnp.float32)
        refs[-1][...] = w_ref[...] * total

    return pl.pallas_call(
        body,
        out_shape=jax.ShapeDtypeStruct(spread.shape, jnp.float32),
        in_specs=[VMEM] * (1 + len(blocks)),
        out_specs=VMEM,
        compiler_params=pltpu.CompilerParams(vmem_limit_bytes=LIMIT),
        cost_estimate=cost(1 << 20, 1 << 20),
        name="finish",
    )(spread, *blocks)


def update(state_ensemble, predicted_data, innovations):
    own = state_ensemble.shape[0] // 8
    x0 = pack_data(predicted_data, innovations)
    p1a = sent(x0, x_turn)
    y0 = sent(x0, y_across)
    s, spread = prepare_state(state_ensemble, own)
    t = sent(s, other_core)
    p1b = sent(x0, x_back)
    p2 = sent(p1a, x_turn)
    q1a = sent(y0, x_turn)
    q1b = sent(y0, x_back)
    y2 = sent(p2, y_across)

    def added(sums, chunks):
        rows = ((s, True, True), (t, True, False), (s, False, True), (t, False, False))
        return add_chunks([(total, *row) for total, row in zip(sums, rows)], chunks)

    sums = added([None] * 4, [x0, p1a])
    sums = added(sums, [y0])
    sums = added(sums, [p1b, p2])
    fs, ft, ns, nt = added(sums, [q1a])
    fs, ft = add_chunks([(fs, s, True, True), (ft, t, True, False)], [q1b], sent_kinds=(1,))
    fh = sent(ft, other_core)
    ns, nt = add_chunks([(ns, s, False, True), (nt, t, False, False)], [q1b], sent_kinds=(1,))
    nh = sent(nt, other_core)
    y2s = sent(y2, other_core)
    (fs,) = add_chunks([(fs, s, True, True)], [y2])
    blocks = {}
    blocks[0, 1], blocks[0, 3] = last_chunks(fs, fh, s, [y2s], own, True, (1, 3))
    blocks[0, 2], kept = last_chunks(fs, fh, s, [y2s], own, True, (2, 0))
    second = last_chunks(ns, nh, s, [y2, y2s], own, False, (2, 1, 3, 0), kept)
    blocks[1, 2], blocks[1, 1], blocks[1, 3], across, mine = second
    last = sent(across, lambda x, y, z, core: (x, y ^ 1, z, core))
    arrived = ([mine], [])
    for (later, k), block in blocks.items():
        arrived[later].append(sent(block, lambda x, y, z, core: (x, y ^ int(core == later), z + k, core)))
    return finish(spread, [early_sum(arrived[0]), *arrived[1], last])


def solution(mesh):
    in_specs = (P("state", None), P(("state", "dp"), None), P(("state", "dp"), None))
    out_specs = P(("state", "dp"), None)
    return jax.shard_map(update, mesh=mesh, in_specs=in_specs, out_specs=out_specs, check_vma=False)
```
